32 devices in a mesh: curve: 8 (over y, x, core), lev: 4 (over z).
Axes of the slice: x: 2, y: 2, z: 4, core: 2. Of those that a mesh axis runs over, the one named last changes fastest.
Arguments:
- source_field: bfloat16 [32768, 1024], P(('curve', 'lev')), may hold values from -6 to 6
- slot_elems: int32 [16, 4096], P(None, ('curve', 'lev')), may hold values from 0 to 1023
- slot_tiles: int32 [4096], P(('curve', 'lev')), may hold values from 0 to 511, as said below
- weights: bfloat16 [4096, 16, 256], P(('curve', 'lev')), may hold values from -0.375 to 0.375
Outputs:
- remapped: float32 [64, 8192], P(None, ('curve', 'lev'))
The draws below stay inside these ranges and needn't reach their ends.
Inputs may be any that keep to these rules, and one draw needn't show every extreme that they name: `slot_elems`: local element ids within the slot's own device's elements. `slot_tiles`: tile g belongs to band g // 64. The 128 slots of a device with curve index b name tiles of the 4 bands b to b + 4 - 1 modulo 8 only, at most 64 of them in one band, a bound reached on every device, and exactly 16 tiles of each residue modulo 8.
All inputs are finite; a program needn't handle non-finite values.
Results may differ from the reference program's by a relative error of at most 0.0003.
Values sent between devices are 32-bit elements; how exact they have to be, the bound alone decides.
A program may use at most 64 MiB of HBM per device.

```python
import jax
import jax.numpy as jnp
from jax import lax

CH = 64
NODE = 16
TILE = 16
EPB = 16
NB = 4
ELEM_DEV = 1024
ELEMS = 32768
CELLS = 8192
TPBAND = 64
NTILE = 512
PER = 8
LB = 128
SLOTS = 4096
N_CURVE = 8
N_LEV = 4


def draw_slot_tiles(key, part):
    count_key = jax.random.fold_in(key, 21)
    shift_key = jax.random.fold_in(key, 22)
    high_key = jax.random.fold_in(key, 23)
    order_key = jax.random.fold_in(key, 24)
    devices = N_CURVE * N_LEV
    counts = jnp.array([LB // 2, LB // 4, LB // 8, LB // 8], dtype=jnp.int32)
    count_order = jax.random.permutation(count_key, NB).astype(jnp.int32)
    device_ids = jnp.arange(devices, dtype=jnp.int32)
    curve_ids = device_ids // N_LEV
    band_steps = jnp.arange(NB, dtype=jnp.int32)
    per_band = counts[count_order[(curve_ids[:, None] + band_steps[None, :]) % NB]]
    band_ends = jnp.cumsum(per_band, axis=1)
    slot_index = jnp.arange(LB, dtype=jnp.int32)
    offset = jnp.sum((slot_index[None, :, None] >= band_ends[:, None, :]).astype(jnp.int32), axis=2)
    band_ids = (curve_ids[:, None] + offset) % N_CURVE
    rshift = jax.random.randint(shift_key, (devices, 1), 0, N_CURVE, dtype=jnp.int32)
    residue = (slot_index[None, :] + rshift) % N_CURVE
    high_part = jax.random.randint(high_key, (devices, LB), 0, PER, dtype=jnp.int32)
    tile_ids = band_ids * TPBAND + high_part * N_CURVE + residue

    def shuffle_order(device_key):
        return jax.random.permutation(device_key, LB)
    orders = jax.vmap(shuffle_order)(jax.random.split(order_key, devices))
    shuffled = jnp.take_along_axis(tile_ids, orders, axis=1)
    return shuffled.reshape(devices * LB).astype(jnp.int32)


def set_ends(entries, own_key, least, top_value):
    place = [jax.random.randint(jax.random.fold_in(own_key, axis), (), 0, length) for axis, length in enumerate(entries.shape)]
    widest = entries.shape.index(max(entries.shape))
    next_to = place[:widest] + [(place[widest] + 1) % entries.shape[widest]] + place[widest + 1:]
    return entries.at[tuple(place)].set(least).at[tuple(next_to)].set(top_value)


def block_scale(key, dims, cuts, least, largest):
    level, own = 1.0, jax.random.fold_in(key, 6)
    for axis_at, blocks in cuts:
        steps = jnp.exp(jax.random.uniform(jax.random.fold_in(own, axis_at), (blocks,), jnp.float32, least / len(cuts), largest / len(cuts)))
        level = level * jnp.repeat(steps, dims[axis_at] // blocks).reshape([-1 if axis == axis_at else 1 for axis in range(len(dims))])
    return level


def bell_draw(own_key, dims, scale, limit, cuts=(), kind=jnp.bfloat16):
    values = jax.random.normal(own_key, dims, jnp.float32) * scale
    if len(cuts) > 0:
        values = block_scale(own_key, dims, cuts, -0.22, 0.18) * values
    return jnp.clip(values, min=-limit, max=limit).astype(kind)


def setup_inputs(seed: int = 0) -> dict:
    key_of = jax.random.split(jax.random.key(seed), 5)
    source_field = bell_draw(key_of[0], (ELEMS, NODE * CH), 1.0, 6.0, ((0, 32),))
    slot_elems = set_ends(jax.random.randint(key_of[1], (EPB, SLOTS), 0, ELEM_DEV), jax.random.fold_in(key_of[1], 1), 0, ELEM_DEV - 1).astype(jnp.int32)
    slot_tiles = draw_slot_tiles(jax.random.fold_in(key_of[4], 71), 0)
    weights = bell_draw(key_of[3], (SLOTS, TILE, EPB * NODE), (EPB * NODE) ** -0.5, 0.375, ((0, 32),))
    return {"source_field": source_field, "slot_elems": slot_elems, "slot_tiles": slot_tiles, "weights": weights}


def reference(source_field, slot_elems, slot_tiles, weights):
    devices = N_CURVE * N_LEV
    row_width = CH * TILE

    def one_device(grid_total, device):
        segment = lax.dynamic_slice_in_dim(source_field, (device * ELEM_DEV).astype(jnp.int32), ELEM_DEV, 0)
        element_ids = lax.dynamic_slice_in_dim(slot_elems, (device * LB).astype(jnp.int32), LB, 1)
        gathered = jnp.take(segment, jnp.transpose(element_ids), axis=0)
        values = gathered.reshape(LB, EPB * NODE, CH)
        slot_weights = lax.dynamic_slice_in_dim(weights, (device * LB).astype(jnp.int32), LB, 0)
        partial_value = jnp.einsum("jnc,jtn->jct", values.astype(jnp.float32), slot_weights.astype(jnp.float32))
        slot_tile_ids = lax.dynamic_slice_in_dim(slot_tiles, (device * LB).astype(jnp.int32), LB, 0)
        grid_total = grid_total.at[slot_tile_ids].add(partial_value.reshape(LB, row_width))
        return grid_total, None

    start_total = jnp.zeros((NTILE, row_width), jnp.float32)
    grid_total, unused = lax.scan(one_device, start_total, jnp.arange(devices, dtype=jnp.int32))
    return jnp.transpose(grid_total.reshape(NTILE, CH, TILE), (1, 0, 2)).reshape(CH, CELLS)
```

```python
import functools

import jax
import jax.numpy as jnp
from jax import lax
from jax.experimental import pallas as pl
from jax.experimental.pallas import tpu as pltpu
from jax.sharding import PartitionSpec as P

NB = 4
CELL_DEV = 256
LANES = 128
SUB = 8
PITCH = SUB + 1
VMEM_GRANT = 40 << 20
MESH = pl.DeviceIdType.MESH
F32 = jnp.float32
BF16 = jnp.bfloat16


class Local:
    def __init__(self, src, elems, tiles, w, bufs, ssem, wsem, isem, esem):
        self.stage, self.wstage, self.tstage, self.estage, self.rows = bufs
        self.esem = esem
        self.pieces = ssem.shape[0]
        self.piece = src.shape[0] // self.pieces
        self.src, self.ssem = src, ssem
        self.weights = pltpu.make_async_copy(w, self.wstage, wsem)
        self.elems = pltpu.make_async_copy(elems, self.estage, isem.at[0])
        self.tiles = pltpu.make_async_copy(tiles, self.tstage, isem.at[1])

    def piece_copy(self, i):
        at = pl.ds(pl.multiple_of(i * self.piece, self.piece), self.piece)
        return pltpu.make_async_copy(self.src.at[at], self.stage.at[at], self.ssem.at[i])

    def row_copy(self, e):
        count = self.estage.shape[1]
        return pltpu.make_async_copy(self.estage.at[e], self.rows.at[pl.ds(e * count, count)], self.esem.at[e])


def local_sums(local, base, total_tiles, acc, table, wd, part, hot):
    stage, wstage, estage, rows = local.stage, local.wstage, local.estage, local.rows
    slot_elems, slot_count = estage.shape
    tile_cells = wstage.shape[0] // slot_count
    half = LANES // 2
    cols = wstage.shape[1]
    piece = local.piece

    local.elems.wait()
    estage[...] = estage[...] * PITCH

    local.tiles.wait()
    rel = local.tstage[...] - base
    rel = jnp.where(rel < 0, rel + total_tiles, rel)
    one = (lax.broadcasted_iota(jnp.int32, (hot.shape[0], slot_count), 0) == rel).astype(F32).astype(BF16)
    hot[:, :slot_count] = one
    hot[:, slot_count:] = one
    for e in range(slot_elems):
        local.row_copy(e).start()

    i = lax.broadcasted_iota(jnp.int32, (cols, cols), 0)
    j = lax.broadcasted_iota(jnp.int32, (cols, cols), 1)
    perm = (i == 2 * (j % (cols // 2)) + j // (cols // 2)).astype(F32).astype(BF16)
    local.weights.wait()

    def permute(i, carry):
        at = pl.ds(pl.multiple_of(i * 256, 256), 256)
        wd[at, :] = jnp.dot(wstage[at, :], perm, preferred_element_type=F32).astype(BF16)
        return carry

    lax.fori_loop(0, wstage.shape[0] // 256, permute, 0)

    def convert_piece(i, carry):
        local.piece_copy(i).wait()

        def convert(n, carry):
            e0 = pl.multiple_of(i * piece + n * 16, 16)
            for pair in range(SUB):
                x = stage[pl.ds(e0, 16), pair * LANES : (pair + 1) * LANES].astype(F32)
                for h in range(2):
                    table[pl.ds((e0 + 8 * h) * PITCH + pair, 8, stride=PITCH), :] = x[8 * h : 8 * h + 8]
            return carry

        return lax.fori_loop(0, piece // 16, convert, carry, unroll=2)

    lax.fori_loop(0, local.pieces, convert_piece, 0)
    for e in range(slot_elems):
        local.row_copy(e).wait()

    low = lax.broadcasted_iota(jnp.int32, (tile_cells, LANES), 1) < half
    group = 16

    def slots(i, carry):
        for u in range(group):
            s = i * group + u
            x = jnp.concatenate(
                [table[pl.ds(rows[e * slot_count + s], SUB), :] for e in range(slot_elems)], axis=0
            ).astype(BF16)
            row = wd[pl.ds(pl.multiple_of(s * tile_cells, tile_cells), tile_cells), :]
            lhs = jnp.concatenate([row[:, : cols // 2], row[:, cols // 2 :]], axis=0)
            r = jnp.dot(lhs, x, preferred_element_type=F32)
            v = jnp.where(low, r[:tile_cells], r[tile_cells:])
            v = v + pltpu.roll(v, half, 1)
            part[pl.ds(s * PITCH, SUB), :] = jnp.where(low[:SUB], v[:SUB], v[SUB:])
        return carry

    lax.fori_loop(0, slot_count // group, slots, 0)

    for t in range(0, SUB, 2):
        sides = []
        for u in range(2):
            x = part[pl.ds(t + u, slot_count, stride=PITCH), :]
            high = x.astype(BF16)
            sides.append(jnp.concatenate([high, (x - high.astype(F32)).astype(BF16)], axis=0))
        r = jnp.dot(hot[...], jnp.concatenate(sides, axis=1), preferred_element_type=F32)
        for u in range(2):
            acc[:, t + u] = r[:, u * LANES : (u + 1) * LANES].reshape(acc.shape[0], acc.shape[2], LANES)


def remap_kernel(
    curve, lev, src, elems, tiles, w, out, acc, stage, wstage, tstage, estage, row_ids, table, wd, part, hot,
    ra, rb, rc, comb, passed, tot, rz, turned, ssem, wsem, isem, esem, asem, bsem, csem, zsem,
):
    b = lax.axis_index("curve")
    l = lax.axis_index("lev")
    p, q = b // 2, b % 2
    odd = p % 2
    pairs = curve // 2
    assert pairs % 2 == 0
    box_tiles = acc.shape[2]
    band_tiles = box_tiles * lev
    detour = odd * (1 - q)
    relay = (1 - odd) * q
    direct = 1 - (1 - odd) * (1 - q)
    partner = p * 2 + (1 - q)
    c_target = lax.rem(p + 2 * q, pairs) * 2 + (1 - q)
    c_source = lax.rem(p - 2 * (1 - q) + 2 * pairs, pairs) * 2 + (1 - q)
    b_source = lax.rem(p - 1 + pairs, pairs) * 2 + q
    d_source = lax.rem(p + 1, pairs) * 2

    local = Local(src, elems, tiles, w, (stage, wstage, tstage, estage, row_ids), ssem, wsem, isem, esem)
    local.elems.start()
    local.tiles.start()
    local.weights.start()

    barrier = pltpu.get_barrier_semaphore()

    def greet(there):
        pl.semaphore_signal(barrier, inc=1, device_id=there, device_id_type=MESH)

    greet((partner, l))
    greet((c_source, l))

    greet((b_source, l))

    @pl.when(relay == 1)
    def _():
        greet((d_source, l))

    for i in range(local.pieces):
        local.piece_copy(i).start()
    for j in range(1, lev):
        greet((b, lax.rem(l + j, lev)))

    local_sums(local, b * band_tiles, curve * band_tiles, acc, table, wd, part, hot)
    pl.semaphore_wait(barrier, 3 + detour + lev - 1)

    def box(j, k=0):
        return k * lev + lax.rem(l + j, lev)

    def copy(src, dst, sems, at, device):
        return pltpu.make_async_remote_copy(
            src_ref=src,
            dst_ref=dst,
            send_sem=sems.at[0, at],
            recv_sem=sems.at[1, at],
            device_id=device,
            device_id_type=MESH,
        )

    parts = 2
    depth = SUB // parts

    def cut(ref, n, at):
        return ref.at[at, pl.ds(n[1] * depth, depth)]

    def slot(n):
        return n[0] * parts + n[1]

    def a_copy(n):
        j = n[0]
        return copy(cut(acc, n, box(j, 3 - 2 * q)), cut(ra, n, box(j)), asem, slot(n), (partner, l))

    def b_copy(n, way):
        target = lax.rem(p + 1 - 2 * way + pairs, pairs) * 2 + q + way
        there = cut(rb, n, box(n[0], way))
        return copy(cut(comb, n, box(n[0])), there, bsem, slot(n) + way * lev * parts, (target, l))

    def c_copy(n, src):
        return copy(src, cut(rc, n, box(n[0])), csem, slot(n), (c_target, l))

    def z_copy(n):
        j = n[0]
        there = (b, lax.rem(l + j, lev))
        return copy(cut(tot, n, box(j)), cut(rz, n, j - 1), zsem, slot(n) - parts, there)

    boxes = sorted(range(1, lev), key=lambda j: -min(j, lev - j)) + [0]
    order = [(j, h) for j in boxes for h in range(parts)]
    first, later = order[:parts], order[parts:]
    for n in order:
        a_copy(n).start()
    for n in first:
        c_copy(n, cut(acc, n, box(n[0], 1 + 2 * q))).start()

    @pl.when(relay == 0)
    def _():
        for n in later:
            c_copy(n, cut(acc, n, box(n[0], 1 + 2 * q))).start()

    for n in order:
        a_copy(n).wait_recv()
        cut(comb, n, box(n[0]))[...] = cut(acc, n, box(n[0], 2))[...] + cut(ra, n, box(n[0]))[...]
        b_copy(n, 0 if n in first else detour).start()

    def pass_on(n):
        @pl.when(relay == 1)
        def _():
            b_copy(n, 1).wait_recv()
            here = cut(passed, n, box(n[0]))
            here[...] = cut(acc, n, box(n[0], 3))[...] + cut(rb, n, box(n[0], 1))[...]
            c_copy(n, here).start()

    def add_direct(n):
        b_copy(n, 0).wait_recv()
        mine = cut(acc, n, box(n[0]))
        mine[...] = mine[...] + cut(rb, n, box(n[0]))[...]

    for i, n in enumerate(order):
        if parts - 1 <= i < len(order) - 1:
            pass_on(order[i + 1])
        if n in first:
            add_direct(n)
        else:
            pl.when(direct == 1)(functools.partial(add_direct, n))
        c_copy(n, cut(passed, n, box(n[0]))).wait_recv()
        cut(tot, n, box(n[0]))[...] = cut(acc, n, box(n[0]))[...] + cut(rc, n, box(n[0]))[...]
        if n[0]:
            z_copy(n).start()
    total = tot[box(0)]
    for j in boxes[:-1]:
        for h in range(parts):
            z_copy((j, h)).wait_recv()
        total = total + rz[j - 1]
    for t in range(SUB):
        turned[pl.ds(t, box_tiles, stride=2 * SUB), :] = total[t]
        turned[pl.ds(SUB + t, box_tiles, stride=2 * SUB), :] = pltpu.roll(total[t], LANES // 2, 1)
    out[...] = jnp.transpose(turned[...])[: out.shape[0]]
    for n in order:
        a_copy(n).wait_send()
        b_copy(n, 0 if n in first else detour).wait_send()
        c_copy(n, cut(passed, n, box(n[0]))).wait_send()
        if n[0]:
            z_copy(n).wait_send()


def per_device(curve, lev, source_field, slot_elems, slot_tiles, weights):
    slot_count, tile_cells, node_cols = weights.shape
    channels = source_field.shape[1] * slot_elems.shape[0] // node_cols
    box_tiles = CELL_DEV // tile_cells
    elem_count = source_field.shape[0]
    vmem = pl.BlockSpec(memory_space=pltpu.VMEM)
    hbm = pl.BlockSpec(memory_space=pl.ANY)
    boxes = pltpu.VMEM((lev, SUB, box_tiles, LANES), F32)
    pieces = 8
    return pl.pallas_call(
        functools.partial(remap_kernel, curve, lev),
        out_shape=jax.ShapeDtypeStruct((channels, CELL_DEV), F32),
        in_specs=[hbm] * 4,
        out_specs=vmem,
        scratch_shapes=[
            pltpu.VMEM((NB * lev, SUB, box_tiles, LANES), F32),
            pltpu.VMEM(source_field.shape, BF16),
            pltpu.VMEM((slot_count * tile_cells, node_cols), BF16),
            pltpu.VMEM((1, slot_count), jnp.int32),
            pltpu.VMEM(slot_elems.shape, jnp.int32),
            pltpu.SMEM((slot_elems.size,), jnp.int32),
            pltpu.VMEM((elem_count * PITCH + SUB, LANES), F32),
            pltpu.VMEM((slot_count * tile_cells, node_cols), BF16),
            pltpu.VMEM((slot_count * PITCH + SUB, LANES), F32),
            pltpu.VMEM((NB * lev * box_tiles, 2 * slot_count), BF16),
        ]
        + [boxes, pltpu.VMEM((2 * lev, SUB, box_tiles, LANES), F32)]
        + [boxes] * 4
        + [
            pltpu.VMEM((lev - 1, SUB, box_tiles, LANES), F32),
            pltpu.VMEM((CELL_DEV, LANES), F32),
            pltpu.SemaphoreType.DMA((pieces,)),
            pltpu.SemaphoreType.DMA,
            pltpu.SemaphoreType.DMA((2,)),
            pltpu.SemaphoreType.DMA((slot_elems.shape[0],)),
            pltpu.SemaphoreType.DMA((2, 2 * lev)),
            pltpu.SemaphoreType.DMA((2, 4 * lev)),
            pltpu.SemaphoreType.DMA((2, 2 * lev)),
            pltpu.SemaphoreType.DMA((2, 2 * lev)),
        ],
        compiler_params=pltpu.CompilerParams(collective_id=0, has_side_effects=True, vmem_limit_bytes=VMEM_GRANT),
        name="remap",
    )(
        *(
            pltpu.with_memory_space_constraint(x, pltpu.HBM)
            for x in (
                source_field,
                slot_elems,
                slot_tiles.reshape(1, slot_count),
                weights.reshape(slot_count * tile_cells, node_cols),
            )
        )
    )


def solution(mesh):
    placed = (
        P(("curve", "lev"), None),
        P(None, ("curve", "lev")),
        P(("curve", "lev")),
        P(("curve", "lev"), None, None),
    )
    return jax.shard_map(
        functools.partial(per_device, mesh.shape["curve"], mesh.shape["lev"]),
        mesh=mesh,
        in_specs=placed,
        out_specs=P(None, ("curve", "lev")),
        check_vma=False,
    )
```

```python
import functools

import jax
import jax.numpy as jnp
from jax import lax
from jax.experimental import pallas as pl
from jax.experimental.pallas import tpu as pltpu
from jax.sharding import PartitionSpec as P

NB = 4
CELL_DEV = 256
LANES = 128
SUB = 8
PITCH = SUB + 1
VMEM_GRANT = 40 << 20
MESH = pl.DeviceIdType.MESH
F32 = jnp.float32
BF16 = jnp.bfloat16


class Local:
    def __init__(self, src, elems, tiles, w, bufs, ssem, wsem, isem, esem):
        self.stage, self.wstage, self.tstage, self.estage, self.rows = bufs
        self.esem = esem
        self.pieces = ssem.shape[0]
        self.piece = src.shape[0] // self.pieces
        self.src, self.ssem = src, ssem
        self.weights = pltpu.make_async_copy(w, self.wstage, wsem)
        self.elems = pltpu.make_async_copy(elems, self.estage, isem.at[0])
        self.tiles = pltpu.make_async_copy(tiles, self.tstage, isem.at[1])

    def piece_copy(self, i):
        at = pl.ds(pl.multiple_of(i * self.piece, self.piece), self.piece)
        return pltpu.make_async_copy(self.src.at[at], self.stage.at[at], self.ssem.at[i])

    def row_copy(self, e):
        count = self.estage.shape[1]
        return pltpu.make_async_copy(self.estage.at[e], self.rows.at[pl.ds(e * count, count)], self.esem.at[e])


def local_sums(local, base, total_tiles, acc, table, wd, part, hot):
    stage, wstage, estage, rows = local.stage, local.wstage, local.estage, local.rows
    slot_elems, slot_count = estage.shape
    tile_cells = wstage.shape[0] // slot_count
    half = LANES // 2
    cols = wstage.shape[1]
    piece = local.piece

    local.elems.wait()
    estage[...] = estage[...] * PITCH

    local.tiles.wait()
    rel = local.tstage[...] - base
    rel = jnp.where(rel < 0, rel + total_tiles, rel)
    one = (lax.broadcasted_iota(jnp.int32, (hot.shape[0], slot_count), 0) == rel).astype(F32).astype(BF16)
    hot[:, :slot_count] = one
    hot[:, slot_count:] = one
    for e in range(slot_elems):
        local.row_copy(e).start()

    i = lax.broadcasted_iota(jnp.int32, (cols, cols), 0)
    j = lax.broadcasted_iota(jnp.int32, (cols, cols), 1)
    perm = (i == 2 * (j % (cols // 2)) + j // (cols // 2)).astype(F32).astype(BF16)
    local.weights.wait()

    for i in range(0, wstage.shape[0], 256):
        wd[i : i + 256, :] = jnp.dot(wstage[i : i + 256, :], perm, preferred_element_type=F32).astype(BF16)

    def convert_piece(i, carry):
        local.piece_copy(i).wait()

        def convert(n, carry):
            e0 = pl.multiple_of(i * piece + n * 16, 16)
            for pair in range(SUB):
                x = stage[pl.ds(e0, 16), pair * LANES : (pair + 1) * LANES].astype(F32)
                for h in range(2):
                    table[pl.ds((e0 + 8 * h) * PITCH + pair, 8, stride=PITCH), :] = x[8 * h : 8 * h + 8]
            return carry

        return lax.fori_loop(0, piece // 16, convert, carry, unroll=2)

    lax.fori_loop(0, local.pieces, convert_piece, 0)
    for e in range(slot_elems):
        local.row_copy(e).wait()

    low = lax.broadcasted_iota(jnp.int32, (tile_cells, LANES), 1) < half
    for s in range(slot_count):
        x = jnp.concatenate(
            [table[pl.ds(rows[e * slot_count + s], SUB), :] for e in range(slot_elems)], axis=0
        ).astype(BF16)
        row = wd[s * tile_cells : (s + 1) * tile_cells, :]
        lhs = jnp.concatenate([row[:, : cols // 2], row[:, cols // 2 :]], axis=0)
        r = jnp.dot(lhs, x, preferred_element_type=F32)
        v = jnp.where(low, r[:tile_cells], r[tile_cells:])
        v = v + pltpu.roll(v, half, 1)
        part[s * PITCH : s * PITCH + SUB, :] = jnp.where(low[:SUB], v[:SUB], v[SUB:])

    for t in range(0, SUB, 2):
        sides = []
        for u in range(2):
            x = part[pl.ds(t + u, slot_count, stride=PITCH), :]
            high = x.astype(BF16)
            sides.append(jnp.concatenate([high, (x - high.astype(F32)).astype(BF16)], axis=0))
        r = jnp.dot(hot[...], jnp.concatenate(sides, axis=1), preferred_element_type=F32)
        for u in range(2):
            acc[:, t + u] = r[:, u * LANES : (u + 1) * LANES].reshape(acc.shape[0], acc.shape[2], LANES)


def remap_kernel(
    curve, lev, src, elems, tiles, w, out, acc, stage, wstage, tstage, estage, row_ids, table, wd, part, hot,
    ra, rb, rc, comb, passed, tot, rz, turned, ssem, wsem, isem, esem, asem, bsem, csem, zsem,
):
    b = lax.axis_index("curve")
    l = lax.axis_index("lev")
    p, q = b // 2, b % 2
    odd = p % 2
    pairs = curve // 2
    assert pairs % 2 == 0
    box_tiles = acc.shape[2]
    band_tiles = box_tiles * lev
    detour = odd * (1 - q)
    relay = (1 - odd) * q
    direct = 1 - (1 - odd) * (1 - q)
    partner = p * 2 + (1 - q)
    c_target = lax.rem(p + 2 * q, pairs) * 2 + (1 - q)
    c_source = lax.rem(p - 2 * (1 - q) + 2 * pairs, pairs) * 2 + (1 - q)
    b_source = lax.rem(p - 1 + pairs, pairs) * 2 + q
    d_source = lax.rem(p + 1, pairs) * 2

    local = Local(src, elems, tiles, w, (stage, wstage, tstage, estage, row_ids), ssem, wsem, isem, esem)
    local.elems.start()
    local.tiles.start()
    local.weights.start()

    barrier = pltpu.get_barrier_semaphore()

    def greet(there):
        pl.semaphore_signal(barrier, inc=1, device_id=there, device_id_type=MESH)

    greet((partner, l))
    greet((c_source, l))

    greet((b_source, l))

    @pl.when(relay == 1)
    def _():
        greet((d_source, l))

    for i in range(local.pieces):
        local.piece_copy(i).start()
    for j in range(1, lev):
        greet((b, lax.rem(l + j, lev)))

    local_sums(local, b * band_tiles, curve * band_tiles, acc, table, wd, part, hot)
    pl.semaphore_wait(barrier, 3 + detour + lev - 1)

    def to_lev(j):
        return j - 1 + (j - 1 >= l).astype(jnp.int32) if j else l

    def box(j, k=0):
        return k * lev + to_lev(j)

    def copy(src, dst, sems, at, device):
        return pltpu.make_async_remote_copy(
            src_ref=src,
            dst_ref=dst,
            send_sem=sems.at[0, at],
            recv_sem=sems.at[1, at],
            device_id=device,
            device_id_type=MESH,
        )

    parts = 2
    depth = SUB // parts

    def cut(ref, n, at):
        return ref.at[at, pl.ds(n[1] * depth, depth)]

    def slot(n):
        return n[0] * parts + n[1]

    def a_copy(n):
        j = n[0]
        return copy(cut(acc, n, box(j, 3 - 2 * q)), cut(ra, n, box(j)), asem, slot(n), (partner, l))

    def b_copy(n, way):
        target = lax.rem(p + 1 - 2 * way + pairs, pairs) * 2 + q + way
        there = cut(rb, n, box(n[0], way))
        return copy(cut(comb, n, box(n[0])), there, bsem, slot(n) + way * lev * parts, (target, l))

    def c_copy(n, src):
        return copy(src, cut(rc, n, box(n[0])), csem, slot(n), (c_target, l))

    def z_copy(n):
        there = to_lev(n[0])
        mine = l - (l > there).astype(jnp.int32)
        return pltpu.make_async_remote_copy(
            src_ref=cut(tot, n, there),
            dst_ref=cut(rz, n, mine),
            send_sem=zsem.at[0, slot(n) - parts],
            recv_sem=zsem.at[1, mine * parts + n[1]],
            device_id=(b, there),
            device_id_type=MESH,
        )

    def z_arrived(n):
        pltpu.make_async_remote_copy(
            src_ref=cut(tot, n, 0),
            dst_ref=cut(rz, n, n[0] - 1),
            send_sem=zsem.at[0, slot(n) - parts],
            recv_sem=zsem.at[1, slot(n) - parts],
            device_id=(b, to_lev(n[0])),
            device_id_type=MESH,
        ).wait_recv()

    boxes = list(range(1, lev)) + [0]
    order = [(j, h) for j in boxes for h in range(parts)]
    first, later = order[:parts], order[parts:]
    for n in order:
        a_copy(n).start()
    for n in first:
        c_copy(n, cut(acc, n, box(n[0], 1 + 2 * q))).start()

    @pl.when(relay == 0)
    def _():
        for n in later:
            c_copy(n, cut(acc, n, box(n[0], 1 + 2 * q))).start()

    for n in order:
        a_copy(n).wait_recv()
        cut(comb, n, box(n[0]))[...] = cut(acc, n, box(n[0], 2))[...] + cut(ra, n, box(n[0]))[...]
        b_copy(n, 0 if n in first else detour).start()

    def pass_on(n):
        @pl.when(relay == 1)
        def _():
            b_copy(n, 1).wait_recv()
            here = cut(passed, n, box(n[0]))
            here[...] = cut(acc, n, box(n[0], 3))[...] + cut(rb, n, box(n[0], 1))[...]
            c_copy(n, here).start()

    def add_direct(n):
        b_copy(n, 0).wait_recv()
        mine = cut(acc, n, box(n[0]))
        mine[...] = mine[...] + cut(rb, n, box(n[0]))[...]

    for i, n in enumerate(order):
        if parts - 1 <= i < len(order) - 1:
            pass_on(order[i + 1])
        if n in first:
            add_direct(n)
        else:
            pl.when(direct == 1)(functools.partial(add_direct, n))
        c_copy(n, cut(passed, n, box(n[0]))).wait_recv()
        cut(tot, n, box(n[0]))[...] = cut(acc, n, box(n[0]))[...] + cut(rc, n, box(n[0]))[...]
        if n[0]:
            z_copy(n).start()
    total = tot[box(0)]
    for j in boxes[:-1]:
        for h in range(parts):
            z_arrived((j, h))
        total = total + rz[j - 1]
    for t in range(SUB):
        turned[pl.ds(t, box_tiles, stride=2 * SUB), :] = total[t]
        turned[pl.ds(SUB + t, box_tiles, stride=2 * SUB), :] = pltpu.roll(total[t], LANES // 2, 1)
    out[...] = jnp.transpose(turned[...])[: out.shape[0]]
    for n in order:
        a_copy(n).wait_send()
        b_copy(n, 0 if n in first else detour).wait_send()
        c_copy(n, cut(passed, n, box(n[0]))).wait_send()
        if n[0]:
            z_copy(n).wait_send()


def per_device(curve, lev, source_field, slot_elems, slot_tiles, weights):
    slot_count, tile_cells, node_cols = weights.shape
    channels = source_field.shape[1] * slot_elems.shape[0] // node_cols
    box_tiles = CELL_DEV // tile_cells
    elem_count = source_field.shape[0]
    vmem = pl.BlockSpec(memory_space=pltpu.VMEM)
    hbm = pl.BlockSpec(memory_space=pl.ANY)
    boxes = pltpu.VMEM((lev, SUB, box_tiles, LANES), F32)
    pieces = 8
    return pl.pallas_call(
        functools.partial(remap_kernel, curve, lev),
        out_shape=jax.ShapeDtypeStruct((channels, CELL_DEV), F32),
        in_specs=[hbm] * 4,
        out_specs=vmem,
        scratch_shapes=[
            pltpu.VMEM((NB * lev, SUB, box_tiles, LANES), F32),
            pltpu.VMEM(source_field.shape, BF16),
            pltpu.VMEM((slot_count * tile_cells, node_cols), BF16),
            pltpu.VMEM((1, slot_count), jnp.int32),
            pltpu.VMEM(slot_elems.shape, jnp.int32),
            pltpu.SMEM((slot_elems.size,), jnp.int32),
            pltpu.VMEM((elem_count * PITCH + SUB, LANES), F32),
            pltpu.VMEM((slot_count * tile_cells, node_cols), BF16),
            pltpu.VMEM((slot_count * PITCH + SUB, LANES), F32),
            pltpu.VMEM((NB * lev * box_tiles, 2 * slot_count), BF16),
        ]
        + [boxes, pltpu.VMEM((2 * lev, SUB, box_tiles, LANES), F32)]
        + [boxes] * 4
        + [
            pltpu.VMEM((lev - 1, SUB, box_tiles, LANES), F32),
            pltpu.VMEM((CELL_DEV, LANES), F32),
            pltpu.SemaphoreType.DMA((pieces,)),
            pltpu.SemaphoreType.DMA,
            pltpu.SemaphoreType.DMA((2,)),
            pltpu.SemaphoreType.DMA((slot_elems.shape[0],)),
            pltpu.SemaphoreType.DMA((2, 2 * lev)),
            pltpu.SemaphoreType.DMA((2, 4 * lev)),
            pltpu.SemaphoreType.DMA((2, 2 * lev)),
            pltpu.SemaphoreType.DMA((2, 2 * lev)),
        ],
        compiler_params=pltpu.CompilerParams(collective_id=0, has_side_effects=True, vmem_limit_bytes=VMEM_GRANT),
        name="remap",
    )(
        *(
            pltpu.with_memory_space_constraint(x, pltpu.HBM)
            for x in (
                source_field,
                slot_elems,
                slot_tiles.reshape(1, slot_count),
                weights.reshape(slot_count * tile_cells, node_cols),
            )
        )
    )


def solution(mesh):
    placed = (
        P(("curve", "lev"), None),
        P(None, ("curve", "lev")),
        P(("curve", "lev")),
        P(("curve", "lev"), None, None),
    )
    return jax.shard_map(
        functools.partial(per_device, mesh.shape["curve"], mesh.shape["lev"]),
        mesh=mesh,
        in_specs=placed,
        out_specs=P(None, ("curve", "lev")),
        check_vma=False,
    )
```

```python
import functools

import jax
import jax.numpy as jnp
from jax import lax
from jax.experimental import pallas as pl
from jax.experimental.pallas import tpu as pltpu
from jax.sharding import PartitionSpec as P

NB = 4
CELL_DEV = 256
LANES = 128
SUB = 8
GROUPS = 2
WORD = 1 << 16
PITCH = SUB + 1
VMEM_GRANT = 40 << 20
MESH = pl.DeviceIdType.MESH
F32 = jnp.float32
BF16 = jnp.bfloat16


class Local:
    def __init__(self, src, elems, tiles, w, bufs, ssem, wsem, isem, esem):
        self.stage, self.wstage, self.tstage, self.estage, self.rows = bufs
        self.pieces = ssem.shape[0]
        self.piece = src.shape[0] // self.pieces
        self.src, self.ssem = src, ssem
        self.weights = pltpu.make_async_copy(w, self.wstage, wsem)
        self.elems = pltpu.make_async_copy(elems, self.estage.at[pl.ds(0, elems.shape[0])], isem.at[0])
        self.tiles = pltpu.make_async_copy(tiles, self.tstage, isem.at[1])
        self.ids = pltpu.make_async_copy(self.estage, self.rows, esem)

    def piece_copy(self, i):
        at = pl.ds(pl.multiple_of(i * self.piece, self.piece), self.piece)
        return pltpu.make_async_copy(self.src.at[at], self.stage.at[at], self.ssem.at[i])


def order_slots(local, base, total_tiles, slot_elems, tile_cells, hot):
    estage = local.estage
    slot_count = estage.shape[1]
    local.elems.wait()
    local.tiles.wait()
    rel = local.tstage[...] - base
    rel = jnp.where(rel < 0, rel + total_tiles, rel)

    square = (slot_count, slot_count)
    row = lax.broadcasted_iota(jnp.int32, square, 0)
    col = lax.broadcasted_iota(jnp.int32, square, 1)

    def total(x):
        while x.shape[0] > SUB:
            x = x[: x.shape[0] // 2] + x[x.shape[0] // 2 :]
        for step in (4, 2, 1):
            x = x + pltpu.roll(x, step, 0)
        return x

    odd = jnp.broadcast_to(rel % GROUPS, (SUB, slot_count))
    before = total(jnp.where(row < col, 1 - jnp.transpose(odd)[:, :1], 0))
    lane = lax.broadcasted_iota(jnp.int32, (SUB, slot_count), 1)
    place = jnp.where(odd == 0, before, slot_count // GROUPS + lane - before)

    pairs = estage[: slot_elems // 2, :] + estage[slot_elems // 2 : slot_elems, :] * WORD
    at = lax.broadcasted_iota(jnp.int32, (SUB, slot_count), 0)
    extra = jnp.where(at == 0, place, lane + rel * WORD)
    keys = jnp.transpose(jnp.concatenate([pairs, extra], axis=0))
    to = keys[:, slot_elems // 2 : slot_elems // 2 + 1] == col
    for e in range(slot_elems // 2):
        ids = total(jnp.where(to, keys[:, e : e + 1], 0))[:1]
        estage[e : e + 1, :] = ids % WORD * PITCH
        estage[slot_elems // 2 + e : slot_elems // 2 + e + 1, :] = ids // WORD * PITCH
    last = slot_elems // 2 + 1
    ids = total(jnp.where(to, keys[:, last : last + 1], 0))
    estage[slot_elems:, :] = ids % WORD
    local.ids.start()

    tile = jnp.broadcast_to(ids[:1] // WORD // GROUPS, hot.shape[1:])
    turn = pltpu.roll(tile, slot_count // GROUPS, 1)
    one = lax.broadcasted_iota(jnp.int32, hot.shape[1:], 0)
    front = lax.broadcasted_iota(jnp.int32, hot.shape[1:], 1) < slot_count // GROUPS
    hot[0] = (one == jnp.where(front, tile, turn)).astype(F32).astype(BF16)
    hot[1] = (one == jnp.where(front, turn, tile)).astype(F32).astype(BF16)


def make_table(local, slot_elems, table, wd):
    stage, wstage = local.stage, local.wstage
    cols = wstage.shape[1]
    piece = local.piece
    i = lax.broadcasted_iota(jnp.int32, (cols, cols), 0)
    j = lax.broadcasted_iota(jnp.int32, (cols, cols), 1)
    perm = (i == 2 * (j % (cols // 2)) + j // (cols // 2)).astype(F32).astype(BF16)
    local.weights.wait()
    tile_cells = wd.shape[1]
    count = 256 // tile_cells
    for i in range(0, wd.shape[0], count):
        block = wstage[i * tile_cells : (i + count) * tile_cells, :]
        block = jnp.dot(block, perm, preferred_element_type=F32).astype(BF16)
        wd[i : i + count] = block.reshape(count, tile_cells, cols)

    def convert_piece(i, carry):
        local.piece_copy(i).wait()

        def convert(n, carry):
            e0 = pl.multiple_of(i * piece + n * 16, 16)
            for pair in range(SUB):
                x = stage[pl.ds(e0, 16), pair * LANES : (pair + 1) * LANES].astype(F32)
                for h in range(2):
                    table[pl.ds((e0 + 8 * h) * PITCH + pair, 8, stride=PITCH), :] = x[8 * h : 8 * h + 8]
            return carry

        return lax.fori_loop(0, piece // 16, convert, carry, unroll=2)

    lax.fori_loop(0, local.pieces, convert_piece, 0)
    local.ids.wait()


def group_sums(local, g, slot_elems, tile_cells, acc, table, wd, part, hot):
    rows = local.rows
    slot_count = local.estage.shape[1]
    cols = wd.shape[2]
    half = LANES // 2
    count = slot_count // GROUPS
    low = lax.broadcasted_iota(jnp.int32, (tile_cells, LANES), 1) < half
    for s in range(g * count, (g + 1) * count):
        x = jnp.concatenate(
            [table[pl.ds(rows[e, s], SUB), :] for e in range(slot_elems)], axis=0
        ).astype(BF16)
        row = wd[rows[slot_elems, s]]
        lhs = jnp.concatenate([row[:, : cols // 2], row[:, cols // 2 :]], axis=0)
        r = jnp.dot(lhs, x, preferred_element_type=F32)
        v = jnp.where(low, r[:tile_cells], r[tile_cells:])
        v = v + pltpu.roll(v, half, 1)
        part[s * PITCH : s * PITCH + SUB, :] = jnp.where(low[:SUB], v[:SUB], v[SUB:])

    for t in range(0, SUB, 2):
        sides = []
        for u in range(2):
            x = part[pl.ds(g * count * PITCH + t + u, count, stride=PITCH), :]
            high = x.astype(BF16)
            sides.append(jnp.concatenate([high, (x - high.astype(F32)).astype(BF16)], axis=0))
        r = jnp.dot(hot[g], jnp.concatenate(sides, axis=1), preferred_element_type=F32)
        for u in range(2):
            acc[g, :, t + u] = r[:, u * LANES : (u + 1) * LANES].reshape(acc.shape[1], acc.shape[3], LANES)


def remap_kernel(
    curve, lev, src, elems, tiles, w, out, acc, stage, wstage, tstage, estage, row_ids, table, wd, part, hot,
    ra, rb, rc, comb, passed, tot, rz, turned, ssem, wsem, isem, esem, asem, bsem, csem, zsem, ready,
):
    b = lax.axis_index("curve")
    l = lax.axis_index("lev")
    p, q = b // 2, b % 2
    odd = p % 2
    pairs = curve // 2
    assert pairs % 2 == 0
    box_tiles = acc.shape[3] * GROUPS
    slot_elems = elems.shape[0]
    tile_cells = w.shape[0] // elems.shape[1]
    band_tiles = box_tiles * lev
    detour = odd * (1 - q)
    relay = (1 - odd) * q
    direct = 1 - (1 - odd) * (1 - q)
    partner = p * 2 + (1 - q)
    c_target = lax.rem(p + 2 * q, pairs) * 2 + (1 - q)
    c_source = lax.rem(p - 2 * (1 - q) + 2 * pairs, pairs) * 2 + (1 - q)
    b_source = lax.rem(p - 1 + pairs, pairs) * 2 + q
    d_source = lax.rem(p + 1, pairs) * 2

    local = Local(src, elems, tiles, w, (stage, wstage, tstage, estage, row_ids), ssem, wsem, isem, esem)
    local.elems.start()
    local.tiles.start()
    local.weights.start()

    barrier = pltpu.get_barrier_semaphore()

    def greet(there):
        pl.semaphore_signal(barrier, inc=1, device_id=there, device_id_type=MESH)

    greet((partner, l))
    greet((c_source, l))

    greet((b_source, l))

    @pl.when(relay == 1)
    def _():
        greet((d_source, l))

    for i in range(local.pieces):
        local.piece_copy(i).start()
    for j in range(1, lev):

        @pl.when(l + j < lev)
        def _():
            greet((b, l + j))

    order_slots(local, b * band_tiles, curve * band_tiles, slot_elems, tile_cells, hot)
    make_table(local, slot_elems, table, wd)
    group_sums(local, 0, slot_elems, tile_cells, acc, table, wd, part, hot)
    pl.semaphore_wait(barrier, 3 + detour + l)
    for j in range(1, lev):

        @pl.when(l - j >= 0)
        def _():
            pl.semaphore_signal(ready.at[l], inc=1, device_id=(b, l - j), device_id_type=MESH)

    def to_lev(j):
        return j - 1 + (j - 1 >= l).astype(jnp.int32) if j else l

    def box(j, k=0):
        return k * lev + to_lev(j)

    def copy(src, dst, sems, at, device):
        return pltpu.make_async_remote_copy(
            src_ref=src,
            dst_ref=dst,
            send_sem=sems.at[0, at],
            recv_sem=sems.at[1, at],
            device_id=device,
            device_id_type=MESH,
        )

    parts = GROUPS

    def cut(ref, n, at):
        return ref.at[n[1], at]

    def slot(n):
        return n[0] * parts + n[1]

    def a_copy(n):
        j = n[0]
        return copy(cut(acc, n, box(j, 3 - 2 * q)), cut(ra, n, box(j)), asem, slot(n), (partner, l))

    def b_copy(n, way):
        target = lax.rem(p + 1 - 2 * way + pairs, pairs) * 2 + q + way
        there = cut(rb, n, box(n[0], way))
        return copy(cut(comb, n, box(n[0])), there, bsem, slot(n) + way * lev * parts, (target, l))

    def c_copy(n, src):
        return copy(src, cut(rc, n, box(n[0])), csem, slot(n), (c_target, l))

    def z_copy(n):
        there = to_lev(n[0])
        mine = l - (l > there).astype(jnp.int32)
        return pltpu.make_async_remote_copy(
            src_ref=cut(tot, n, there),
            dst_ref=cut(rz, n, mine),
            send_sem=zsem.at[0, slot(n) - parts],
            recv_sem=zsem.at[1, mine * parts + n[1]],
            device_id=(b, there),
            device_id_type=MESH,
        )

    def z_arrived(n):
        pltpu.make_async_remote_copy(
            src_ref=cut(tot, n, 0),
            dst_ref=cut(rz, n, n[0] - 1),
            send_sem=zsem.at[0, slot(n) - parts],
            recv_sem=zsem.at[1, slot(n) - parts],
            device_id=(b, to_lev(n[0])),
            device_id_type=MESH,
        ).wait_recv()

    boxes = list(range(1, lev)) + [0]
    order = [(j, h) for j in boxes for h in range(parts)]
    first, later = order[:parts], order[parts:]

    def send(h):
        some = [n for n in order if n[1] == h]
        for n in some:
            a_copy(n).start()
        for n in some:
            if n in first:
                c_copy(n, cut(acc, n, box(n[0], 1 + 2 * q))).start()

        @pl.when(relay == 0)
        def _():
            for n in some:
                if n in later:
                    c_copy(n, cut(acc, n, box(n[0], 1 + 2 * q))).start()

    send(0)
    for h in range(1, parts):
        group_sums(local, h, slot_elems, tile_cells, acc, table, wd, part, hot)
        send(h)

    for n in order:
        a_copy(n).wait_recv()
        cut(comb, n, box(n[0]))[...] = cut(acc, n, box(n[0], 2))[...] + cut(ra, n, box(n[0]))[...]
        b_copy(n, 0 if n in first else detour).start()

    def pass_on(n):
        @pl.when(relay == 1)
        def _():
            b_copy(n, 1).wait_recv()
            here = cut(passed, n, box(n[0]))
            here[...] = cut(acc, n, box(n[0], 3))[...] + cut(rb, n, box(n[0], 1))[...]
            c_copy(n, here).start()

    def add_direct(n):
        b_copy(n, 0).wait_recv()
        mine = cut(acc, n, box(n[0]))
        mine[...] = mine[...] + cut(rb, n, box(n[0]))[...]

    for i, n in enumerate(order):
        if parts - 1 <= i < len(order) - 1:
            pass_on(order[i + 1])
        if n in first:
            add_direct(n)
        else:
            pl.when(direct == 1)(functools.partial(add_direct, n))
        c_copy(n, cut(passed, n, box(n[0]))).wait_recv()
        cut(tot, n, box(n[0]))[...] = cut(acc, n, box(n[0]))[...] + cut(rc, n, box(n[0]))[...]
        if n[0]:
            if n[1] == 0:

                @pl.when(to_lev(n[0]) > l)
                def _():
                    pl.semaphore_wait(ready.at[to_lev(n[0])], 1)

            z_copy(n).start()
    for h in range(parts):
        total = tot[h, l]
        for j in boxes[:-1]:
            z_arrived((j, h))
            total = total + rz[h, j - 1]
        for t in range(SUB):
            at, step = h * 2 * SUB + t, parts * 2 * SUB
            turned[pl.ds(at, box_tiles // parts, stride=step), :] = total[t]
            turned[pl.ds(at + SUB, box_tiles // parts, stride=step), :] = pltpu.roll(total[t], LANES // 2, 1)
    out[...] = jnp.transpose(turned[...])[: out.shape[0]]
    for n in order:
        a_copy(n).wait_send()
        b_copy(n, 0 if n in first else detour).wait_send()
        c_copy(n, cut(passed, n, box(n[0]))).wait_send()
        if n[0]:
            z_copy(n).wait_send()


def per_device(curve, lev, source_field, slot_elems, slot_tiles, weights):
    slot_count, tile_cells, node_cols = weights.shape
    channels = source_field.shape[1] * slot_elems.shape[0] // node_cols
    box_tiles = CELL_DEV // tile_cells
    elem_count = source_field.shape[0]
    vmem = pl.BlockSpec(memory_space=pltpu.VMEM)
    hbm = pl.BlockSpec(memory_space=pl.ANY)
    half_box = (SUB, box_tiles // GROUPS, LANES)
    boxes = pltpu.VMEM((GROUPS, lev, *half_box), F32)
    pieces = 8
    return pl.pallas_call(
        functools.partial(remap_kernel, curve, lev),
        out_shape=jax.ShapeDtypeStruct((channels, CELL_DEV), F32),
        in_specs=[hbm] * 4,
        out_specs=vmem,
        scratch_shapes=[
            pltpu.VMEM((GROUPS, NB * lev, *half_box), F32),
            pltpu.VMEM(source_field.shape, BF16),
            pltpu.VMEM((slot_count * tile_cells, node_cols), BF16),
            pltpu.VMEM((1, slot_count), jnp.int32),
            pltpu.VMEM((slot_elems.shape[0] + SUB, slot_count), jnp.int32),
            pltpu.SMEM((slot_elems.shape[0] + SUB, slot_count), jnp.int32),
            pltpu.VMEM((elem_count * PITCH + SUB, LANES), F32),
            pltpu.VMEM((slot_count, tile_cells, node_cols), BF16),
            pltpu.VMEM((slot_count * PITCH + SUB, LANES), F32),
            pltpu.VMEM((GROUPS, NB * lev * box_tiles // GROUPS, slot_count), BF16),
        ]
        + [boxes, pltpu.VMEM((GROUPS, 2 * lev, *half_box), F32)]
        + [boxes] * 4
        + [
            pltpu.VMEM((GROUPS, lev - 1, *half_box), F32),
            pltpu.VMEM((CELL_DEV, LANES), F32),
            pltpu.SemaphoreType.DMA((pieces,)),
            pltpu.SemaphoreType.DMA,
            pltpu.SemaphoreType.DMA((2,)),
            pltpu.SemaphoreType.DMA,
            pltpu.SemaphoreType.DMA((2, 2 * lev)),
            pltpu.SemaphoreType.DMA((2, 4 * lev)),
            pltpu.SemaphoreType.DMA((2, 2 * lev)),
            pltpu.SemaphoreType.DMA((2, 2 * lev)),
            pltpu.SemaphoreType.REGULAR((lev,)),
        ],
        compiler_params=pltpu.CompilerParams(collective_id=0, has_side_effects=True, vmem_limit_bytes=VMEM_GRANT),
        name="remap",
    )(
        *(
            pltpu.with_memory_space_constraint(x, pltpu.HBM)
            for x in (
                source_field,
                slot_elems,
                slot_tiles.reshape(1, slot_count),
                weights.reshape(slot_count * tile_cells, node_cols),
            )
        )
    )


def solution(mesh):
    placed = (
        P(("curve", "lev"), None),
        P(None, ("curve", "lev")),
        P(("curve", "lev")),
        P(("curve", "lev"), None, None),
    )
    return jax.shard_map(
        functools.partial(per_device, mesh.shape["curve"], mesh.shape["lev"]),
        mesh=mesh,
        in_specs=placed,
        out_specs=P(None, ("curve", "lev")),
        check_vma=False,
    )
```

```python
import functools

import jax
import jax.numpy as jnp
from jax import lax
from jax.experimental import pallas as pl
from jax.experimental.pallas import tpu as pltpu
from jax.sharding import PartitionSpec as P

NB = 4
CELL_DEV = 256
LANES = 128
SUB = 8
GROUPS = 2
WORD = 1 << 16
PITCH = SUB + 1
VMEM_GRANT = 40 << 20
MESH = pl.DeviceIdType.MESH
F32 = jnp.float32
BF16 = jnp.bfloat16


class Local:
    def __init__(self, src, elems, tiles, w, bufs, ssem, wsem, isem, esem):
        self.stage, self.wstage, self.tstage, self.estage, self.rows = bufs
        self.pieces = ssem.shape[0]
        self.piece = src.shape[0] // self.pieces
        self.src, self.ssem = src, ssem
        self.weights = pltpu.make_async_copy(w, self.wstage, wsem)
        self.elems = pltpu.make_async_copy(elems, self.estage.at[pl.ds(0, elems.shape[0])], isem.at[0])
        self.tiles = pltpu.make_async_copy(tiles, self.tstage, isem.at[1])
        self.ids = pltpu.make_async_copy(self.estage, self.rows, esem)

    def piece_copy(self, i):
        at = pl.ds(pl.multiple_of(i * self.piece, self.piece), self.piece)
        return pltpu.make_async_copy(self.src.at[at], self.stage.at[at], self.ssem.at[i])


def order_slots(local, base, total_tiles, slot_elems, tile_cells, hot):
    estage = local.estage
    slot_count = estage.shape[1]
    local.elems.wait()
    local.tiles.wait()
    rel = local.tstage[...] - base
    rel = jnp.where(rel < 0, rel + total_tiles, rel)

    square = (slot_count, slot_count)
    row = lax.broadcasted_iota(jnp.int32, square, 0)
    col = lax.broadcasted_iota(jnp.int32, square, 1)

    def total(x):
        while x.shape[0] > SUB:
            x = x[: x.shape[0] // 2] + x[x.shape[0] // 2 :]
        for step in (4, 2, 1):
            x = x + pltpu.roll(x, step, 0)
        return x

    odd = jnp.broadcast_to(rel % GROUPS, (SUB, slot_count))
    before = total(jnp.where(row < col, 1 - jnp.transpose(odd)[:, :1], 0))
    lane = lax.broadcasted_iota(jnp.int32, (SUB, slot_count), 1)
    place = jnp.where(odd == 0, before, slot_count // GROUPS + lane - before)

    pairs = estage[: slot_elems // 2, :] + estage[slot_elems // 2 : slot_elems, :] * WORD
    at = lax.broadcasted_iota(jnp.int32, (SUB, slot_count), 0)
    extra = jnp.where(at == 0, place, lane + rel * WORD)
    keys = jnp.transpose(jnp.concatenate([pairs, extra], axis=0))
    to = keys[:, slot_elems // 2 : slot_elems // 2 + 1] == col
    for e in range(slot_elems // 2):
        ids = total(jnp.where(to, keys[:, e : e + 1], 0))[:1]
        estage[e : e + 1, :] = ids % WORD * PITCH
        estage[slot_elems // 2 + e : slot_elems // 2 + e + 1, :] = ids // WORD * PITCH
    last = slot_elems // 2 + 1
    ids = total(jnp.where(to, keys[:, last : last + 1], 0))
    estage[slot_elems:, :] = ids % WORD
    local.ids.start()

    tile = jnp.broadcast_to(ids[:1] // WORD // GROUPS, hot.shape[1:])
    turn = pltpu.roll(tile, slot_count // GROUPS, 1)
    one = lax.broadcasted_iota(jnp.int32, hot.shape[1:], 0)
    front = lax.broadcasted_iota(jnp.int32, hot.shape[1:], 1) < slot_count // GROUPS
    hot[0] = (one == jnp.where(front, tile, turn)).astype(F32).astype(BF16)
    hot[1] = (one == jnp.where(front, turn, tile)).astype(F32).astype(BF16)


def make_table(local, slot_elems, table, wd):
    stage, wstage = local.stage, local.wstage
    cols = wstage.shape[1]
    piece = local.piece
    i = lax.broadcasted_iota(jnp.int32, (cols, cols), 0)
    j = lax.broadcasted_iota(jnp.int32, (cols, cols), 1)
    perm = (i == 2 * (j % (cols // 2)) + j // (cols // 2)).astype(F32).astype(BF16)
    local.weights.wait()
    tile_cells = wd.shape[1]
    count = 256 // tile_cells
    for i in range(0, wd.shape[0], count):
        block = wstage[i * tile_cells : (i + count) * tile_cells, :]
        block = jnp.dot(block, perm, preferred_element_type=F32).astype(BF16)
        wd[i : i + count] = block.reshape(count, tile_cells, cols)

    def convert_piece(i, carry):
        local.piece_copy(i).wait()

        def convert(n, carry):
            e0 = pl.multiple_of(i * piece + n * 16, 16)
            for pair in range(SUB):
                x = stage[pl.ds(e0, 16), pair * LANES : (pair + 1) * LANES].astype(F32)
                for h in range(2):
                    table[pl.ds((e0 + 8 * h) * PITCH + pair, 8, stride=PITCH), :] = x[8 * h : 8 * h + 8]
            return carry

        return lax.fori_loop(0, piece // 16, convert, carry, unroll=2)

    lax.fori_loop(0, local.pieces, convert_piece, 0)
    local.ids.wait()


def group_sums(local, g, slot_elems, tile_cells, acc, table, wd, part, hot):
    rows = local.rows
    slot_count = local.estage.shape[1]
    cols = wd.shape[2]
    half = LANES // 2
    count = slot_count // GROUPS
    low = lax.broadcasted_iota(jnp.int32, (tile_cells, LANES), 1) < half
    for s in range(g * count, (g + 1) * count):
        x = jnp.concatenate(
            [table[pl.ds(rows[e, s], SUB), :] for e in range(slot_elems)], axis=0
        ).astype(BF16)
        row = wd[rows[slot_elems, s]]
        lhs = jnp.concatenate([row[:, : cols // 2], row[:, cols // 2 :]], axis=0)
        r = jnp.dot(lhs, x, preferred_element_type=F32)
        v = jnp.where(low, r[:tile_cells], r[tile_cells:])
        v = v + pltpu.roll(v, half, 1)
        part[s * PITCH : s * PITCH + SUB, :] = jnp.where(low[:SUB], v[:SUB], v[SUB:])

    for t in range(0, SUB, 2):
        sides = []
        for u in range(2):
            x = part[pl.ds(g * count * PITCH + t + u, count, stride=PITCH), :]
            high = x.astype(BF16)
            sides.append(jnp.concatenate([high, (x - high.astype(F32)).astype(BF16)], axis=0))
        r = jnp.dot(hot[g], jnp.concatenate(sides, axis=1), preferred_element_type=F32)
        for u in range(2):
            acc[g, :, t + u] = r[:, u * LANES : (u + 1) * LANES].reshape(acc.shape[1], acc.shape[3], LANES)


def remap_kernel(
    curve, lev, src, elems, tiles, w, out, acc, stage, wstage, tstage, estage, row_ids, table, wd, part, hot,
    ra, rb, rc, comb, passed, tot, rz, turned, ssem, wsem, isem, esem, asem, bsem, csem, zsem, ready,
):
    b = lax.axis_index("curve")
    l = lax.axis_index("lev")
    p, q = b // 2, b % 2
    odd = p % 2
    pairs = curve // 2
    assert pairs % 2 == 0
    box_tiles = acc.shape[3] * GROUPS
    slot_elems = elems.shape[0]
    tile_cells = w.shape[0] // elems.shape[1]
    band_tiles = box_tiles * lev
    detour = odd * (1 - q)
    relay = (1 - odd) * q
    direct = 1 - (1 - odd) * (1 - q)
    partner = p * 2 + (1 - q)
    c_target = lax.rem(p + 2 * q, pairs) * 2 + (1 - q)
    c_source = lax.rem(p - 2 * (1 - q) + 2 * pairs, pairs) * 2 + (1 - q)
    b_source = lax.rem(p - 1 + pairs, pairs) * 2 + q
    d_source = lax.rem(p + 1, pairs) * 2

    local = Local(src, elems, tiles, w, (stage, wstage, tstage, estage, row_ids), ssem, wsem, isem, esem)
    local.elems.start()
    local.tiles.start()
    local.weights.start()

    barrier = pltpu.get_barrier_semaphore()

    def greet(there):
        pl.semaphore_signal(barrier, inc=1, device_id=there, device_id_type=MESH)

    greet((partner, l))
    greet((c_source, l))

    greet((b_source, l))

    @pl.when(relay == 1)
    def _():
        greet((d_source, l))

    for i in range(local.pieces):
        local.piece_copy(i).start()
    for j in range(1, lev):

        @pl.when(l + j < lev)
        def _():
            greet((b, l + j))

    order_slots(local, b * band_tiles, curve * band_tiles, slot_elems, tile_cells, hot)
    make_table(local, slot_elems, table, wd)
    group_sums(local, 0, slot_elems, tile_cells, acc, table, wd, part, hot)
    pl.semaphore_wait(barrier, 3 + detour + l)
    for j in range(1, lev):

        @pl.when(l - j >= 0)
        def _():
            pl.semaphore_signal(ready.at[l], inc=1, device_id=(b, l - j), device_id_type=MESH)

    def to_lev(j):
        return jnp.where(l == 0, lev - j, j - 1 + (j - 1 >= l).astype(jnp.int32)) if j else l

    def box(j, k=0):
        return k * lev + to_lev(j)

    def copy(src, dst, sems, at, device):
        return pltpu.make_async_remote_copy(
            src_ref=src,
            dst_ref=dst,
            send_sem=sems.at[0, at],
            recv_sem=sems.at[1, at],
            device_id=device,
            device_id_type=MESH,
        )

    parts = GROUPS

    def cut(ref, n, at):
        return ref.at[n[1], at]

    def slot(n):
        return n[0] * parts + n[1]

    def a_copy(n):
        j = n[0]
        return copy(cut(acc, n, box(j, 3 - 2 * q)), cut(ra, n, box(j)), asem, slot(n), (partner, l))

    def b_copy(n, way):
        target = lax.rem(p + 1 - 2 * way + pairs, pairs) * 2 + q + way
        there = cut(rb, n, box(n[0], way))
        return copy(cut(comb, n, box(n[0])), there, bsem, slot(n) + way * lev * parts, (target, l))

    def c_copy(n, src):
        return copy(src, cut(rc, n, box(n[0])), csem, slot(n), (c_target, l))

    def z_copy(n):
        there = to_lev(n[0])
        mine = l - (l > there).astype(jnp.int32)
        return pltpu.make_async_remote_copy(
            src_ref=cut(tot, n, there),
            dst_ref=cut(rz, n, mine),
            send_sem=zsem.at[0, slot(n) - parts],
            recv_sem=zsem.at[1, mine * parts + n[1]],
            device_id=(b, there),
            device_id_type=MESH,
        )

    def z_arrived(n):
        pltpu.make_async_remote_copy(
            src_ref=cut(tot, n, 0),
            dst_ref=cut(rz, n, n[0] - 1),
            send_sem=zsem.at[0, slot(n) - parts],
            recv_sem=zsem.at[1, slot(n) - parts],
            device_id=(b, to_lev(n[0])),
            device_id_type=MESH,
        ).wait_recv()

    boxes = list(range(1, lev)) + [0]
    order = [(j, h) for j in boxes for h in range(parts)]
    first, later = order[:parts], order[parts:]

    def send(h):
        some = [n for n in order if n[1] == h]
        for n in some:
            a_copy(n).start()
        for n in some:
            if n in first:
                c_copy(n, cut(acc, n, box(n[0], 1 + 2 * q))).start()

        @pl.when(relay == 0)
        def _():
            for n in some:
                if n in later:
                    c_copy(n, cut(acc, n, box(n[0], 1 + 2 * q))).start()

    send(0)
    for h in range(1, parts):
        group_sums(local, h, slot_elems, tile_cells, acc, table, wd, part, hot)
        send(h)

    for n in order:
        a_copy(n).wait_recv()
        cut(comb, n, box(n[0]))[...] = cut(acc, n, box(n[0], 2))[...] + cut(ra, n, box(n[0]))[...]
        b_copy(n, 0 if n in first else detour).start()

    def pass_on(n):
        @pl.when(relay == 1)
        def _():
            b_copy(n, 1).wait_recv()
            here = cut(passed, n, box(n[0]))
            here[...] = cut(acc, n, box(n[0], 3))[...] + cut(rb, n, box(n[0], 1))[...]
            c_copy(n, here).start()

    def add_direct(n):
        b_copy(n, 0).wait_recv()
        mine = cut(acc, n, box(n[0]))
        mine[...] = mine[...] + cut(rb, n, box(n[0]))[...]

    for i, n in enumerate(order):
        if parts - 1 <= i < len(order) - 1:
            pass_on(order[i + 1])
        if n in first:
            add_direct(n)
        else:
            pl.when(direct == 1)(functools.partial(add_direct, n))
        c_copy(n, cut(passed, n, box(n[0]))).wait_recv()
        cut(tot, n, box(n[0]))[...] = cut(acc, n, box(n[0]))[...] + cut(rc, n, box(n[0]))[...]
        if n[0]:
            if n[1] == 0:

                @pl.when(to_lev(n[0]) > l)
                def _():
                    pl.semaphore_wait(ready.at[to_lev(n[0])], 1)

            z_copy(n).start()
    for h in range(parts):
        total = tot[h, l]
        for j in boxes[:-1]:
            z_arrived((j, h))
            total = total + rz[h, j - 1]
        for t in range(SUB):
            at, step = h * 2 * SUB + t, parts * 2 * SUB
            turned[pl.ds(at, box_tiles // parts, stride=step), :] = total[t]
            turned[pl.ds(at + SUB, box_tiles // parts, stride=step), :] = pltpu.roll(total[t], LANES // 2, 1)
    out[...] = jnp.transpose(turned[...])[: out.shape[0]]
    for n in order:
        a_copy(n).wait_send()
        b_copy(n, 0 if n in first else detour).wait_send()
        c_copy(n, cut(passed, n, box(n[0]))).wait_send()
        if n[0]:
            z_copy(n).wait_send()


def per_device(curve, lev, source_field, slot_elems, slot_tiles, weights):
    slot_count, tile_cells, node_cols = weights.shape
    channels = source_field.shape[1] * slot_elems.shape[0] // node_cols
    box_tiles = CELL_DEV // tile_cells
    elem_count = source_field.shape[0]
    vmem = pl.BlockSpec(memory_space=pltpu.VMEM)
    hbm = pl.BlockSpec(memory_space=pl.ANY)
    half_box = (SUB, box_tiles // GROUPS, LANES)
    boxes = pltpu.VMEM((GROUPS, lev, *half_box), F32)
    pieces = 8
    return pl.pallas_call(
        functools.partial(remap_kernel, curve, lev),
        out_shape=jax.ShapeDtypeStruct((channels, CELL_DEV), F32),
        in_specs=[hbm] * 4,
        out_specs=vmem,
        scratch_shapes=[
            pltpu.VMEM((GROUPS, NB * lev, *half_box), F32),
            pltpu.VMEM(source_field.shape, BF16),
            pltpu.VMEM((slot_count * tile_cells, node_cols), BF16),
            pltpu.VMEM((1, slot_count), jnp.int32),
            pltpu.VMEM((slot_elems.shape[0] + SUB, slot_count), jnp.int32),
            pltpu.SMEM((slot_elems.shape[0] + SUB, slot_count), jnp.int32),
            pltpu.VMEM((elem_count * PITCH + SUB, LANES), F32),
            pltpu.VMEM((slot_count, tile_cells, node_cols), BF16),
            pltpu.VMEM((slot_count * PITCH + SUB, LANES), F32),
            pltpu.VMEM((GROUPS, NB * lev * box_tiles // GROUPS, slot_count), BF16),
        ]
        + [boxes, pltpu.VMEM((GROUPS, 2 * lev, *half_box), F32)]
        + [boxes] * 4
        + [
            pltpu.VMEM((GROUPS, lev - 1, *half_box), F32),
            pltpu.VMEM((CELL_DEV, LANES), F32),
            pltpu.SemaphoreType.DMA((pieces,)),
            pltpu.SemaphoreType.DMA,
            pltpu.SemaphoreType.DMA((2,)),
            pltpu.SemaphoreType.DMA,
            pltpu.SemaphoreType.DMA((2, 2 * lev)),
            pltpu.SemaphoreType.DMA((2, 4 * lev)),
            pltpu.SemaphoreType.DMA((2, 2 * lev)),
            pltpu.SemaphoreType.DMA((2, 2 * lev)),
            pltpu.SemaphoreType.REGULAR((lev,)),
        ],
        compiler_params=pltpu.CompilerParams(collective_id=0, has_side_effects=True, vmem_limit_bytes=VMEM_GRANT),
        name="remap",
    )(
        *(
            pltpu.with_memory_space_constraint(x, pltpu.HBM)
            for x in (
                source_field,
                slot_elems,
                slot_tiles.reshape(1, slot_count),
                weights.reshape(slot_count * tile_cells, node_cols),
            )
        )
    )


def solution(mesh):
    placed = (
        P(("curve", "lev"), None),
        P(None, ("curve", "lev")),
        P(("curve", "lev")),
        P(("curve", "lev"), None, None),
    )
    return jax.shard_map(
        functools.partial(per_device, mesh.shape["curve"], mesh.shape["lev"]),
        mesh=mesh,
        in_specs=placed,
        out_specs=P(None, ("curve", "lev")),
        check_vma=False,
    )
```

```python
import functools

import jax
import jax.numpy as jnp
from jax import lax
from jax.experimental import pallas as pl
from jax.experimental.pallas import tpu as pltpu
from jax.sharding import PartitionSpec as P

NB = 4
CELL_DEV = 256
LANES = 128
SUB = 8
GROUPS = 2
WORD = 1 << 16
PITCH = SUB + 1
VMEM_GRANT = 40 << 20
MESH = pl.DeviceIdType.MESH
F32 = jnp.float32
BF16 = jnp.bfloat16


class Local:
    def __init__(self, src, elems, tiles, w, bufs, ssem, wsem, isem, esem):
        self.stage, self.wstage, self.tstage, self.estage, self.rows = bufs
        self.pieces = ssem.shape[0]
        self.piece = src.shape[0] // self.pieces
        self.src, self.ssem = src, ssem
        self.weights = pltpu.make_async_copy(w, self.wstage, wsem)
        self.elems = pltpu.make_async_copy(elems, self.estage.at[pl.ds(0, elems.shape[0])], isem.at[0])
        self.tiles = pltpu.make_async_copy(tiles, self.tstage, isem.at[1])
        self.ids = pltpu.make_async_copy(self.estage, self.rows, esem)

    def piece_copy(self, i):
        at = pl.ds(pl.multiple_of(i * self.piece, self.piece), self.piece)
        return pltpu.make_async_copy(self.src.at[at], self.stage.at[at], self.ssem.at[i])


def order_slots(local, base, total_tiles, slot_elems, tile_cells, hot):
    estage = local.estage
    slot_count = estage.shape[1]
    local.elems.wait()
    local.tiles.wait()
    rel = local.tstage[...] - base
    rel = jnp.where(rel < 0, rel + total_tiles, rel)

    square = (slot_count, slot_count)
    row = lax.broadcasted_iota(jnp.int32, square, 0)
    col = lax.broadcasted_iota(jnp.int32, square, 1)

    def total(x):
        while x.shape[0] > SUB:
            x = x[: x.shape[0] // 2] + x[x.shape[0] // 2 :]
        for step in (4, 2, 1):
            x = x + pltpu.roll(x, step, 0)
        return x

    odd = jnp.broadcast_to(rel % GROUPS, (SUB, slot_count))
    before = total(jnp.where(row < col, 1 - jnp.transpose(odd)[:, :1], 0))
    lane = lax.broadcasted_iota(jnp.int32, (SUB, slot_count), 1)
    place = jnp.where(odd == 0, before, slot_count // GROUPS + lane - before)

    pairs = estage[: slot_elems // 2, :] + estage[slot_elems // 2 : slot_elems, :] * WORD
    at = lax.broadcasted_iota(jnp.int32, (SUB, slot_count), 0)
    extra = jnp.where(at == 0, place, lane + rel * WORD)
    keys = jnp.transpose(jnp.concatenate([pairs, extra], axis=0))
    to = keys[:, slot_elems // 2 : slot_elems // 2 + 1] == col
    for e in range(slot_elems // 2):
        ids = total(jnp.where(to, keys[:, e : e + 1], 0))[:1]
        estage[e : e + 1, :] = ids % WORD * PITCH
        estage[slot_elems // 2 + e : slot_elems // 2 + e + 1, :] = ids // WORD * PITCH
    last = slot_elems // 2 + 1
    ids = total(jnp.where(to, keys[:, last : last + 1], 0))
    estage[slot_elems:, :] = ids % WORD
    local.ids.start()

    tile = jnp.broadcast_to(ids[:1] // WORD // GROUPS, hot.shape[1:])
    turn = pltpu.roll(tile, slot_count // GROUPS, 1)
    one = lax.broadcasted_iota(jnp.int32, hot.shape[1:], 0)
    front = lax.broadcasted_iota(jnp.int32, hot.shape[1:], 1) < slot_count // GROUPS
    hot[0] = (one == jnp.where(front, tile, turn)).astype(F32).astype(BF16)
    hot[1] = (one == jnp.where(front, turn, tile)).astype(F32).astype(BF16)


def make_table(local, slot_elems, table, wd):
    stage, wstage = local.stage, local.wstage
    cols = wstage.shape[1]
    piece = local.piece
    i = lax.broadcasted_iota(jnp.int32, (cols, cols), 0)
    j = lax.broadcasted_iota(jnp.int32, (cols, cols), 1)
    perm = (i == 2 * (j % (cols // 2)) + j // (cols // 2)).astype(F32).astype(BF16)
    local.weights.wait()
    tile_cells = wd.shape[1]
    count = 256 // tile_cells
    for i in range(0, wd.shape[0], count):
        block = wstage[i * tile_cells : (i + count) * tile_cells, :]
        block = jnp.dot(block, perm, preferred_element_type=F32).astype(BF16)
        wd[i : i + count] = block.reshape(count, tile_cells, cols)

    def convert_piece(i, carry):
        local.piece_copy(i).wait()

        def convert(n, carry):
            e0 = pl.multiple_of(i * piece + n * 16, 16)
            for pair in range(SUB):
                x = stage[pl.ds(e0, 16), pair * LANES : (pair + 1) * LANES].astype(F32)
                for h in range(2):
                    table[pl.ds((e0 + 8 * h) * PITCH + pair, 8, stride=PITCH), :] = x[8 * h : 8 * h + 8]
            return carry

        return lax.fori_loop(0, piece // 16, convert, carry, unroll=2)

    lax.fori_loop(0, local.pieces, convert_piece, 0)
    local.ids.wait()


def group_sums(local, g, slot_elems, tile_cells, acc, table, wd, part, hot):
    rows = local.rows
    slot_count = local.estage.shape[1]
    cols = wd.shape[2]
    half = LANES // 2
    count = slot_count // GROUPS
    low = lax.broadcasted_iota(jnp.int32, (tile_cells, LANES), 1) < half
    for s in range(g * count, (g + 1) * count):
        x = jnp.concatenate(
            [table[pl.ds(rows[e, s], SUB), :] for e in range(slot_elems)], axis=0
        ).astype(BF16)
        row = wd[rows[slot_elems, s]]
        lhs = jnp.concatenate([row[:, : cols // 2], row[:, cols // 2 :]], axis=0)
        r = jnp.dot(lhs, x, preferred_element_type=F32)
        v = jnp.where(low, r[:tile_cells], r[tile_cells:])
        v = v + pltpu.roll(v, half, 1)
        part[s * PITCH : s * PITCH + SUB, :] = jnp.where(low[:SUB], v[:SUB], v[SUB:])

    for t in range(0, SUB, 2):
        sides = []
        for u in range(2):
            x = part[pl.ds(g * count * PITCH + t + u, count, stride=PITCH), :]
            high = x.astype(BF16)
            sides.append(jnp.concatenate([high, (x - high.astype(F32)).astype(BF16)], axis=0))
        r = jnp.dot(hot[g], jnp.concatenate(sides, axis=1), preferred_element_type=F32)
        for u in range(2):
            acc[g, :, t + u] = r[:, u * LANES : (u + 1) * LANES].reshape(acc.shape[1], acc.shape[3], LANES)


def remap_kernel(
    curve, lev, src, elems, tiles, w, out, acc, stage, wstage, tstage, estage, row_ids, table, wd, part, hot,
    ra, rb, rc, comb, passed, tot, rz, turned, ssem, wsem, isem, esem, asem, bsem, csem, zsem, ready,
):
    b = lax.axis_index("curve")
    l = lax.axis_index("lev")
    p, q = b // 2, b % 2
    odd = p % 2
    pairs = curve // 2
    assert pairs % 2 == 0
    box_tiles = acc.shape[3] * GROUPS
    slot_elems = elems.shape[0]
    tile_cells = w.shape[0] // elems.shape[1]
    band_tiles = box_tiles * lev
    detour = odd * (1 - q)
    relay = (1 - odd) * q
    direct = 1 - (1 - odd) * (1 - q)
    partner = p * 2 + (1 - q)
    c_target = lax.rem(p + 2 * q, pairs) * 2 + (1 - q)
    c_source = lax.rem(p - 2 * (1 - q) + 2 * pairs, pairs) * 2 + (1 - q)
    b_source = lax.rem(p - 1 + pairs, pairs) * 2 + q
    d_source = lax.rem(p + 1, pairs) * 2

    local = Local(src, elems, tiles, w, (stage, wstage, tstage, estage, row_ids), ssem, wsem, isem, esem)
    local.elems.start()
    local.tiles.start()
    local.weights.start()

    barrier = pltpu.get_barrier_semaphore()

    def greet(there):
        pl.semaphore_signal(barrier, inc=1, device_id=there, device_id_type=MESH)

    greet((partner, l))
    greet((c_source, l))

    greet((b_source, l))

    @pl.when(relay == 1)
    def _():
        greet((d_source, l))

    for i in range(local.pieces):
        local.piece_copy(i).start()
    for j in range(1, lev):

        @pl.when(l + j < lev)
        def _():
            greet((b, l + j))

    order_slots(local, b * band_tiles, curve * band_tiles, slot_elems, tile_cells, hot)
    make_table(local, slot_elems, table, wd)
    group_sums(local, 0, slot_elems, tile_cells, acc, table, wd, part, hot)
    pl.semaphore_wait(barrier, 3 + detour + l)
    for j in range(1, lev):

        @pl.when(l - j >= 0)
        def _():
            pl.semaphore_signal(ready.at[l], inc=1, device_id=(b, l - j), device_id_type=MESH)

    def to_lev(j):
        if not j:
            return l
        rising = j - 1 + (j - 1 >= l).astype(jnp.int32)
        falling = 0 if j == 1 else lev + 1 - j - (lev + 1 - j <= l).astype(jnp.int32)
        return jnp.where(l == 0, lev - j, jnp.where(l < lev // 2, falling, rising))

    def box(j, k=0):
        return k * lev + to_lev(j)

    def copy(src, dst, sems, at, device):
        return pltpu.make_async_remote_copy(
            src_ref=src,
            dst_ref=dst,
            send_sem=sems.at[0, at],
            recv_sem=sems.at[1, at],
            device_id=device,
            device_id_type=MESH,
        )

    parts = GROUPS

    def cut(ref, n, at):
        return ref.at[n[1], at]

    def slot(n):
        return n[0] * parts + n[1]

    def a_copy(n):
        j = n[0]
        return copy(cut(acc, n, box(j, 3 - 2 * q)), cut(ra, n, box(j)), asem, slot(n), (partner, l))

    def b_copy(n, way):
        target = lax.rem(p + 1 - 2 * way + pairs, pairs) * 2 + q + way
        there = cut(rb, n, box(n[0], way))
        return copy(cut(comb, n, box(n[0])), there, bsem, slot(n) + way * lev * parts, (target, l))

    def c_copy(n, src):
        return copy(src, cut(rc, n, box(n[0])), csem, slot(n), (c_target, l))

    def z_copy(n):
        there = to_lev(n[0])
        mine = l - (l > there).astype(jnp.int32)
        return pltpu.make_async_remote_copy(
            src_ref=cut(tot, n, there),
            dst_ref=cut(rz, n, mine),
            send_sem=zsem.at[0, slot(n) - parts],
            recv_sem=zsem.at[1, mine * parts + n[1]],
            device_id=(b, there),
            device_id_type=MESH,
        )

    def z_arrived(n):
        pltpu.make_async_remote_copy(
            src_ref=cut(tot, n, 0),
            dst_ref=cut(rz, n, n[0] - 1),
            send_sem=zsem.at[0, slot(n) - parts],
            recv_sem=zsem.at[1, slot(n) - parts],
            device_id=(b, to_lev(n[0])),
            device_id_type=MESH,
        ).wait_recv()

    boxes = list(range(1, lev)) + [0]
    order = [(j, h) for j in boxes for h in range(parts)]
    first, later = order[:parts], order[parts:]

    def send(h):
        some = [n for n in order if n[1] == h]
        for n in some:
            a_copy(n).start()
        for n in some:
            if n in first:
                c_copy(n, cut(acc, n, box(n[0], 1 + 2 * q))).start()

        @pl.when(relay == 0)
        def _():
            for n in some:
                if n in later:
                    c_copy(n, cut(acc, n, box(n[0], 1 + 2 * q))).start()

    send(0)
    for h in range(1, parts):
        group_sums(local, h, slot_elems, tile_cells, acc, table, wd, part, hot)
        send(h)

    for n in order:
        a_copy(n).wait_recv()
        cut(comb, n, box(n[0]))[...] = cut(acc, n, box(n[0], 2))[...] + cut(ra, n, box(n[0]))[...]
        b_copy(n, 0 if n in first else detour).start()

    def pass_on(n):
        @pl.when(relay == 1)
        def _():
            b_copy(n, 1).wait_recv()
            here = cut(passed, n, box(n[0]))
            here[...] = cut(acc, n, box(n[0], 3))[...] + cut(rb, n, box(n[0], 1))[...]
            c_copy(n, here).start()

    def add_direct(n):
        b_copy(n, 0).wait_recv()
        mine = cut(acc, n, box(n[0]))
        mine[...] = mine[...] + cut(rb, n, box(n[0]))[...]

    for i, n in enumerate(order):
        if parts - 1 <= i < len(order) - 1:
            pass_on(order[i + 1])
        if n in first:
            add_direct(n)
        else:
            pl.when(direct == 1)(functools.partial(add_direct, n))
        c_copy(n, cut(passed, n, box(n[0]))).wait_recv()
        cut(tot, n, box(n[0]))[...] = cut(acc, n, box(n[0]))[...] + cut(rc, n, box(n[0]))[...]
        if n[0]:
            if n[1] == 0:

                @pl.when(to_lev(n[0]) > l)
                def _():
                    pl.semaphore_wait(ready.at[to_lev(n[0])], 1)

            z_copy(n).start()
    for h in range(parts):
        total = tot[h, l]
        for j in boxes[:-1]:
            z_arrived((j, h))
            total = total + rz[h, j - 1]
        for t in range(SUB):
            at, step = h * 2 * SUB + t, parts * 2 * SUB
            turned[pl.ds(at, box_tiles // parts, stride=step), :] = total[t]
            turned[pl.ds(at + SUB, box_tiles // parts, stride=step), :] = pltpu.roll(total[t], LANES // 2, 1)
    out[...] = jnp.transpose(turned[...])[: out.shape[0]]
    for n in order:
        a_copy(n).wait_send()
        b_copy(n, 0 if n in first else detour).wait_send()
        c_copy(n, cut(passed, n, box(n[0]))).wait_send()
        if n[0]:
            z_copy(n).wait_send()


def per_device(curve, lev, source_field, slot_elems, slot_tiles, weights):
    slot_count, tile_cells, node_cols = weights.shape
    channels = source_field.shape[1] * slot_elems.shape[0] // node_cols
    box_tiles = CELL_DEV // tile_cells
    elem_count = source_field.shape[0]
    vmem = pl.BlockSpec(memory_space=pltpu.VMEM)
    hbm = pl.BlockSpec(memory_space=pl.ANY)
    half_box = (SUB, box_tiles // GROUPS, LANES)
    boxes = pltpu.VMEM((GROUPS, lev, *half_box), F32)
    pieces = 8
    return pl.pallas_call(
        functools.partial(remap_kernel, curve, lev),
        out_shape=jax.ShapeDtypeStruct((channels, CELL_DEV), F32),
        in_specs=[hbm] * 4,
        out_specs=vmem,
        scratch_shapes=[
            pltpu.VMEM((GROUPS, NB * lev, *half_box), F32),
            pltpu.VMEM(source_field.shape, BF16),
            pltpu.VMEM((slot_count * tile_cells, node_cols), BF16),
            pltpu.VMEM((1, slot_count), jnp.int32),
            pltpu.VMEM((slot_elems.shape[0] + SUB, slot_count), jnp.int32),
            pltpu.SMEM((slot_elems.shape[0] + SUB, slot_count), jnp.int32),
            pltpu.VMEM((elem_count * PITCH + SUB, LANES), F32),
            pltpu.VMEM((slot_count, tile_cells, node_cols), BF16),
            pltpu.VMEM((slot_count * PITCH + SUB, LANES), F32),
            pltpu.VMEM((GROUPS, NB * lev * box_tiles // GROUPS, slot_count), BF16),
        ]
        + [boxes, pltpu.VMEM((GROUPS, 2 * lev, *half_box), F32)]
        + [boxes] * 4
        + [
            pltpu.VMEM((GROUPS, lev - 1, *half_box), F32),
            pltpu.VMEM((CELL_DEV, LANES), F32),
            pltpu.SemaphoreType.DMA((pieces,)),
            pltpu.SemaphoreType.DMA,
            pltpu.SemaphoreType.DMA((2,)),
            pltpu.SemaphoreType.DMA,
            pltpu.SemaphoreType.DMA((2, 2 * lev)),
            pltpu.SemaphoreType.DMA((2, 4 * lev)),
            pltpu.SemaphoreType.DMA((2, 2 * lev)),
            pltpu.SemaphoreType.DMA((2, 2 * lev)),
            pltpu.SemaphoreType.REGULAR((lev,)),
        ],
        compiler_params=pltpu.CompilerParams(collective_id=0, has_side_effects=True, vmem_limit_bytes=VMEM_GRANT),
        name="remap",
    )(
        *(
            pltpu.with_memory_space_constraint(x, pltpu.HBM)
            for x in (
                source_field,
                slot_elems,
                slot_tiles.reshape(1, slot_count),
                weights.reshape(slot_count * tile_cells, node_cols),
            )
        )
    )


def solution(mesh):
    placed = (
        P(("curve", "lev"), None),
        P(None, ("curve", "lev")),
        P(("curve", "lev")),
        P(("curve", "lev"), None, None),
    )
    return jax.shard_map(
        functools.partial(per_device, mesh.shape["curve"], mesh.shape["lev"]),
        mesh=mesh,
        in_specs=placed,
        out_specs=P(None, ("curve", "lev")),
        check_vma=False,
    )
```
